256 devices in a mesh: replica: 4 (over y), fsdp: 16 (over z, core), tensor: 4 (over x).
Axes of the slice: x: 4, y: 4, z: 8, core: 2. Of those that a mesh axis runs over, the one named last changes fastest.
Arguments:
- attn_out: bfloat16 [16384, 8192], P(('replica', 'tensor'), 'fsdp'), may hold values from -6 to 6
- out_grad: bfloat16 [16384, 8192], P(('replica', 'fsdp'), 'tensor'), may hold values from -0.09375 to 0.09375
- error_in: float32 [4, 8192, 8192], P('replica', 'fsdp', 'tensor'), may hold values from -4 to 4
- factor_in: float32 [8192, 32], P('tensor'), may hold values from -0.0625 to 0.0625
Outputs:
- new_error: float32 [4, 8192, 8192], P('replica', 'fsdp', 'tensor')
- update: bfloat16 [8192, 8192], P('fsdp', 'tensor')
- new_factor: float32 [8192, 32], P('tensor')
The draws below stay inside these ranges and needn't reach their ends.
All inputs are finite; a program needn't handle non-finite values.
Results may differ from the reference program's by a relative error of at most 0.001.
Values may be sent and summed in bfloat16 or wider, within the bound.
No kernel may reach another device: no remote copies, remote signals or barrier semaphores. Data moves between devices by JAX's collectives and lax.ppermute only.
A program may use at most 128 MiB of HBM per device.

```python
import jax
import jax.numpy as jnp
from jax import lax

DIN = 8192
DOUT = 8192
RANK = 32
TOK = 4096
TOK_ALL = 16384
N_REPLICA = 4


def shard_levels(own_key, shape, cuts, least, high):
    factor_of, own = 1.0, jax.random.fold_in(own_key, 6)
    for axis_at, parts in cuts:
        steps = jnp.exp(jax.random.uniform(jax.random.fold_in(own, axis_at), (parts,), jnp.float32, least / len(cuts), high / len(cuts)))
        factor_of = factor_of * jnp.repeat(steps, shape[axis_at] // parts).reshape([-1 if axis == axis_at else 1 for axis in range(len(shape))])
    return factor_of


def centred(rng, extent, deviation, reach, cuts=(), kind=jnp.bfloat16):
    drawn = jax.random.normal(rng, extent, jnp.float32) * deviation
    if len(cuts) > 0:
        drawn = shard_levels(rng, extent, cuts, -0.22, 0.18) * drawn
    return jnp.clip(drawn, min=-reach, max=reach).astype(kind)


def setup_inputs(seed: int = 0) -> dict:
    arg_keys = jax.random.split(jax.random.key(seed), 5)
    return {
        "attn_out": centred(arg_keys[0], (TOK_ALL, DIN), 1.0, 6.0, ((0, 16), (1, 16))),
        "out_grad": centred(arg_keys[1], (TOK_ALL, DOUT), TOK ** -0.5, 0.09375, ((0, 64), (1, 4))),
        "error_in": centred(arg_keys[2], (N_REPLICA, DIN, DOUT), 0.5, 4.0, ((0, 4), (1, 16), (2, 4)), jnp.float32),
        "factor_in": centred(arg_keys[3], (DOUT, RANK), DOUT ** -0.5, 0.0625, ((0, 4),), jnp.float32),
    }


def reference(attn_out, out_grad, error_in, factor_in):
    tokens = attn_out.shape[0] // N_REPLICA
    activations = attn_out.reshape(N_REPLICA, tokens, DIN)
    cotangents = out_grad.reshape(N_REPLICA, tokens, DOUT)

    def per_replica(items):
        act_block, cot_block, memory = items
        return jnp.dot(act_block.T.astype(jnp.float32), cot_block.astype(jnp.float32), preferred_element_type=jnp.float32) + memory
    merged = lax.map(per_replica, (activations, cotangents, error_in))
    left = jnp.einsum('rij,jk->ik', merged, factor_in, precision=lax.Precision.HIGHEST) / N_REPLICA
    gram_matrix = jnp.dot(left.T, left, precision=lax.Precision.HIGHEST)
    triangle = jnp.linalg.cholesky(gram_matrix)
    orthonormal = jax.scipy.linalg.solve_triangular(triangle, left.T, lower=True).T
    new_factor = jnp.einsum('rij,ik->jk', merged, orthonormal, precision=lax.Precision.HIGHEST) / N_REPLICA
    decompressed = jnp.dot(orthonormal, new_factor.T, precision=lax.Precision.HIGHEST)
    new_error = merged - decompressed[None]
    return (new_error, decompressed.astype(jnp.bfloat16), new_factor)
```

```python
import jax
import jax.numpy as jnp
from jax import lax
from jax.sharding import PartitionSpec as P


RANK = 32


def split2(v):
    hi = lax.reduce_precision(v, 8, 7)
    lo = v - hi
    return hi.astype(jnp.bfloat16), lax.reduce_precision(lo, 8, 7).astype(jnp.bfloat16)


def thin(lhs, rhs, lhs_dim):
    hi, lo = split2(rhs)
    both = lax.dot_general(
        lhs,
        jnp.concatenate([hi, lo], axis=1),
        (((lhs_dim,), (0,)), ((), ())),
        preferred_element_type=jnp.float32,
    )
    return both[:, :RANK] + both[:, RANK:]


def all_sent(parts, axis):
    return lax.all_to_all(parts, axis, 0, 0, tiled=True)


def copies(shard, axis):
    return jnp.broadcast_to(shard, (lax.axis_size(axis), *shard.shape))


def body(attn_out, out_grad, error_in, factor_in):
    n_f = lax.axis_size("fsdp")
    n_x = lax.axis_size("tensor")
    n_y = lax.axis_size("replica")
    n_z = n_f // 2
    memory = error_in[0]
    f_at = lax.axis_index("fsdp")
    x_at = lax.axis_index("tensor")
    z_at, c_at = f_at // 2, f_at % 2
    own_rows = attn_out.shape[0]
    g_rows = out_grad.shape[0]

    def z_step(v, by):
        pairs = [(2 * z + c, 2 * ((z + by) % n_z) + c) for z in range(n_z) for c in range(2)]
        return lax.ppermute(v, "fsdp", pairs)

    def sibling(v):
        return lax.ppermute(v, "fsdp", [(f, f ^ 1) for f in range(n_f)])

    def x_step(v, by):
        return lax.ppermute(v, "tensor", [(i, (i + by) % n_x) for i in range(n_x)])

    projected = thin(out_grad, factor_in, 1)
    everyone = all_sent(copies(projected, "fsdp"), "fsdp")
    quarter = all_sent(everyone.reshape(n_x, own_rows, RANK), "tensor").sum(axis=0)
    from_memory = jnp.dot(memory, factor_in, precision=lax.Precision.HIGH)
    partial_left = thin(attn_out, quarter, 0) + from_memory
    left = all_sent(copies(partial_left, ("replica", "tensor")), ("replica", "tensor")).sum(axis=0) / n_y

    half = own_rows // 2
    up, down = x_step(attn_out, 1), x_step(attn_out, -1)
    far_top, far_bottom = x_step(up[:half], 1), x_step(down[half:], -1)
    acts = jnp.zeros((n_x * own_rows, attn_out.shape[1]), attn_out.dtype)
    acts = lax.dynamic_update_slice(acts, attn_out, (x_at * own_rows, 0))
    acts = lax.dynamic_update_slice(acts, up, ((x_at + 3) % 4 * own_rows, 0))
    acts = lax.dynamic_update_slice(acts, down, ((x_at + 1) % 4 * own_rows, 0))
    acts = lax.dynamic_update_slice(acts, far_top, ((x_at + 2) % 4 * own_rows, 0))
    acts = lax.dynamic_update_slice(acts, far_bottom, ((x_at + 2) % 4 * own_rows + half, 0))

    q_part = thin(acts, left, 1).reshape(n_f, g_rows, RANK)
    gram_part = jnp.dot(left.T, left, precision=lax.Precision.HIGHEST)
    sent = jnp.concatenate([q_part, copies(gram_part, "fsdp")], axis=1)
    summed = all_sent(sent, "fsdp").sum(axis=0)
    q_own, gram = summed[:g_rows], summed[g_rows:]
    triangle = jnp.linalg.cholesky(gram)
    inverse = jax.scipy.linalg.solve_triangular(triangle, jnp.eye(RANK, dtype=jnp.float32), lower=True)
    orthonormal = jnp.dot(left, inverse.T, precision=lax.Precision.HIGHEST)
    p_local = thin(out_grad, q_own, 0) + lax.dot_general(
        memory, left, (((0,), (0,)), ((), ())), precision=lax.Precision.HIGH
    )
    group = ("replica", "fsdp")
    n_g = n_y * n_f
    piece = all_sent(p_local.reshape(n_g, -1, RANK), group).sum(axis=0)
    p_all = all_sent(copies(piece, group), group).reshape(p_local.shape) / n_y
    new_factor = jnp.dot(p_all, inverse.T, precision=lax.Precision.HIGHEST)

    total = memory

    def fold(total, block, z_of, c_of):
        rows = lax.dynamic_slice(acts, (z_of * 2 * g_rows + c_of * g_rows, 0), (g_rows, acts.shape[1]))
        return total + lax.dot_general(
            rows, block, (((0,), (0,)), ((), ())), preferred_element_type=jnp.float32
        )

    hg = g_rows // 2
    top, bottom = out_grad[:hg], out_grad[hg:]
    blocks = [(out_grad, 0)]
    cw, ccw = [top, bottom], [top, bottom]
    for s in range(1, n_z // 2):
        cw = [z_step(v, 1) for v in cw]
        ccw = [z_step(v, -1) for v in ccw]
        blocks.append((jnp.concatenate(cw), -s))
        blocks.append((jnp.concatenate(ccw), s))
    last = jnp.concatenate([z_step(cw[0], 1), z_step(ccw[1], -1)])
    blocks.append((last, n_z // 2))
    for block, by in blocks:
        z_of = (z_at + by + n_z) % n_z
        total = fold(total, block, z_of, c_at)
        total = fold(total, sibling(block), z_of, 1 - c_at)

    o_hi, o_lo = split2(orthonormal)
    n_hi, n_lo = split2(new_factor)
    decompressed = lax.dot_general(
        jnp.concatenate([o_hi, o_hi, o_lo], axis=1),
        jnp.concatenate([n_hi, n_lo, n_hi], axis=1),
        (((1,), (1,)), ((), ())),
        preferred_element_type=jnp.float32,
    )
    new_error = (total - decompressed)[None]
    return (new_error, decompressed.astype(jnp.bfloat16), new_factor)


def solution(mesh):
    placed = (
        P(("replica", "tensor"), "fsdp"),
        P(("replica", "fsdp"), "tensor"),
        P("replica", "fsdp", "tensor"),
        P("tensor", None),
    )
    return jax.shard_map(
        body,
        mesh=mesh,
        in_specs=placed,
        out_specs=(P("replica", "fsdp", "tensor"), P("fsdp", "tensor"), P("tensor", None)),
        check_vma=False,
    )
```

```python
import functools

import jax
import jax.numpy as jnp
from jax import lax
from jax.experimental import pallas as pl
from jax.experimental.pallas import tpu as pltpu
from jax.sharding import PartitionSpec as P


RANK = 32
F32, BF16 = jnp.float32, jnp.bfloat16
NN, NT = (((1,), (0,)), ((), ())), (((1,), (1,)), ((), ()))
VMEM = pl.BlockSpec(memory_space=pltpu.VMEM)
SMEM = pl.BlockSpec(memory_space=pltpu.SMEM)


def dot(a, b, dims, precision=None):
    return lax.dot_general(a, b, dims, precision=precision, preferred_element_type=F32)


def hi_lo(v):
    hi = v.astype(BF16)
    return hi, (v - hi.astype(F32)).astype(BF16)


def stacked(v):
    return jnp.concatenate(hi_lo(v), axis=0)


def halves(v):
    return v[:RANK] + v[RANK:]


def kernel(fn, out, specs, flops=0, moved=0, **more):
    return pl.pallas_call(
        fn,
        out_shape=out,
        in_specs=specs,
        cost_estimate=pl.CostEstimate(flops=flops, bytes_accessed=moved, transcendentals=0),
        compiler_params=pltpu.CompilerParams(vmem_limit_bytes=56 * 2**20),
        **more,
    )


def shape(*dims, of=F32):
    return jax.ShapeDtypeStruct(dims, of)


def seat(at_ref):
    code = at_ref[0]
    return code // 64, code // 8 % 8, code // 4 % 2, code % 4


def part_of(at_ref, by):
    _, z, _, x = seat(at_ref)
    chip = (z + by + 8) % 8
    near = (chip // 2 - x + 4) % 4
    return jnp.where(near == 0, 0, jnp.where(near == 3, 2, jnp.where(near == 1, 4, 6))) + chip % 2


def turn_halves(a_ref, *outs):
    rows = a_ref.shape[0] // 2
    for i, out in enumerate(outs):
        out[...] = a_ref[i * rows : (i + 1) * rows, :].T


def project(f_ref, g_ref, out_ref):
    part = halves(dot(stacked(f_ref[...]), g_ref[...], NT))
    for i in range(out_ref.shape[0]):
        out_ref[i] = part


def sum_copies(in_ref, *refs):
    out_ref = refs[-1]
    total = in_ref[0]
    for i in range(1, in_ref.shape[0]):
        total += in_ref[i]
    for i in range(out_ref.shape[0]):
        out_ref[i] = total


def memory_right(f_ref, e_ref, out_ref):
    hi, lo = hi_lo(e_ref[...])
    both = stacked(f_ref[...])
    out_ref[...] = halves(dot(both, hi, NT)) + dot(both[:RANK], lo, NT)


def left_terms(at_ref, q_ref, s_ref, m_ref, *refs):
    out_ref = refs[-1]
    south = seat(at_ref)[2] == 0
    total = m_ref[...]
    for k in range(q_ref.shape[0]):
        mine, other = q_ref[k], s_ref[k]
        both = [jnp.where(south, mine, other), jnp.where(south, other, mine)]
        total += halves(dot(stacked(jnp.concatenate(both, axis=1)), refs[k][...], NT))
    for i in range(out_ref.shape[0]):
        out_ref[i] = total


def gram_terms(n_y, l_ref, left_ref, out_ref):
    left = sum(l_ref[i] for i in range(l_ref.shape[0])) / n_y
    left_ref[...] = left
    gram = dot(left, left, NT, lax.Precision.HIGHEST)
    packed = jnp.concatenate([gram[8 * j : 8 * j + 8] for j in range(RANK // 8)], axis=1)
    for i in range(out_ref.shape[0]):
        out_ref[i] = packed


def gram_sum(in_ref, out_ref):
    packed = sum(in_ref[i] for i in range(in_ref.shape[0]))
    out_ref[...] = jnp.concatenate(
        [packed[:, RANK * j : RANK * (j + 1)] for j in range(RANK // 8)], axis=0
    )


def pick(at_ref, by, parts, out, column, left_ref):
    which = part_of(at_ref, by)
    rows, width = parts[0].shape
    both = stacked(left_ref[...])
    for k, part in enumerate(parts):

        @pl.when(which == k)
        def _():
            out[:rows, column : column + width] = part[...]
            terms = stacked(halves(dot(both, part[...], NN)))
            out[rows:, column : column + width] = terms


def packed_in(at_ref, flips, blocks, packed):
    core = seat(at_ref)[2]
    rows = blocks[0].shape[0]
    for j, (flip, block) in enumerate(zip(flips, blocks)):
        side = 1 - core if flip else core
        first = pl.multiple_of(j // 2 * 2 * rows + side * rows, rows)
        packed[pl.ds(first, rows), :] = block[...]


def fold(bys, flips, late, at_ref, c_ref, left_ref, *refs):
    parts, blocks = refs[:8], refs[8 : 8 + len(flips)]
    out_ref, p_ref, ended, turned, packed = refs[8 + len(flips) :]
    rows, width = parts[0].shape

    @pl.when(pl.program_id(0) == 0)
    def _():
        back = 2 * seat(at_ref)[2] - 1
        for j, by in enumerate(bys):
            pick(at_ref, by * back, parts, turned, j * width, left_ref)
        for j, by in enumerate(late):
            pick(at_ref, by * back, parts, ended, j * width, left_ref)

    packed_in(at_ref, flips, blocks, packed)
    memory = c_ref[...]
    out_ref[...] = memory + dot(turned[:rows, :], packed[...], NN)
    hi, lo = hi_lo(memory)
    both = stacked(left_ref[...])
    p_ref[...] = (
        halves(dot(turned[rows:, :], packed[...], NN))
        + halves(dot(both, hi, NN))
        + dot(both[:RANK], lo, NN)
    )


def last_terms(flips, at_ref, p_ref, turned, *refs):
    blocks, (piece_ref, packed) = refs[:-2], refs[-2:]
    packed_in(at_ref, flips, blocks, packed)
    p = p_ref[...] + halves(dot(turned[-2 * RANK :, :], packed[...], NN))
    across = p.shape[1] // 128
    for r in range(RANK // 8):
        for j in range(across):
            piece_ref[r * across + j] = p[8 * r : 8 * r + 8, 128 * j : 128 * j + 128]


def fold_last(flips, at_ref, c_ref, turned, *refs):
    blocks, (out_ref, packed) = refs[:-2], refs[-2:]
    packed_in(at_ref, flips, blocks, packed)
    out_ref[...] = c_ref[...] + dot(turned[: c_ref.shape[0], :], packed[...], NN)


def finish(n_y, c_ref, o_ref, inv_ref, p_ref, error_ref, update_ref, factor_ref):
    across = p_ref.shape[1] // (RANK // 8)
    p = jnp.concatenate(
        [
            jnp.concatenate([p_ref[0, r * across + j] for j in range(across)], axis=1)
            for r in range(RANK // 8)
        ],
        axis=0,
    )
    factor = dot(inv_ref[...], p, NN, lax.Precision.HIGHEST) / n_y
    factor_ref[...] = factor
    hi, lo = hi_lo(factor)
    lifted = dot(o_ref[...], jnp.concatenate([hi, lo, hi], axis=0), NN)
    update_ref[...] = lifted.astype(BF16)
    error_ref[...] = c_ref[...] - lifted


def body(attn_out, out_grad, error_in, factor_in):
    n_z = lax.axis_size("z")
    n_f = 2 * n_z
    fsdp = ("z", "core")
    n_x = lax.axis_size("tensor")
    n_y = lax.axis_size("replica")
    memory = error_in[0]
    x_at = lax.axis_index("tensor")
    z_at, c_at = lax.axis_index("z"), lax.axis_index("core")
    own_rows, d_in = attn_out.shape
    g_rows, d_out = out_grad.shape
    half = own_rows // 2
    code = ((lax.axis_index("replica") * n_z + z_at) * 2 + c_at) * n_x + x_at
    code = code.reshape(1).astype(jnp.int32)

    def all_sent(parts, axis):
        return lax.all_to_all(parts, axis, 0, 0, tiled=True)

    def turn(v):
        pairs = [(2 * z, 2 * ((z + 1) % n_z)) for z in range(n_z)]
        pairs += [(2 * z + 1, 2 * ((z - 1) % n_z) + 1) for z in range(n_z)]
        return lax.ppermute(v, fsdp, pairs)

    def sibling(v):
        return lax.ppermute(v, "core", [(0, 1), (1, 0)])

    def x_step(v, by):
        return lax.ppermute(v, "tensor", [(i, (i + by) % n_x) for i in range(n_x)])

    factor_t = factor_in.T
    projected = kernel(
        project, shape(n_x, RANK, g_rows), [VMEM] * 2, flops=2 * 64 * g_rows * d_out
    )(factor_t, out_grad)
    projected = all_sent(projected, "tensor")
    own = kernel(
        turn_halves, (shape(d_in, half, of=BF16),) * 2, [VMEM], flops=64 * own_rows * d_in
    )(attn_out)
    projected = kernel(sum_copies, shape(n_z, RANK, g_rows), [VMEM])(projected)
    everyone = all_sent(projected, "z")
    per = n_f // n_x
    mine = lax.dynamic_slice_in_dim(everyone, x_at * (per // 2), per // 2)
    theirs = sibling(mine)
    memory_f = kernel(
        memory_right,
        shape(RANK, d_in),
        [
            pl.BlockSpec((RANK, d_out), lambda n: (0, 0)),
            pl.BlockSpec((128, d_out), lambda n: (n, 0)),
        ],
        flops=2 * 96 * d_in * d_out,
        grid=(d_in // 128,),
        out_specs=pl.BlockSpec((RANK, 128), lambda n: (0, n)),
    )(factor_t, memory)
    left_part = kernel(
        left_terms,
        shape(n_y * n_x, RANK, d_in),
        [SMEM] + [VMEM] * 5,
        flops=2 * 64 * own_rows * d_in,
    )(code, mine, theirs, memory_f, *own)
    left_parts = all_sent(left_part, ("replica", "tensor"))

    up = [x_step(own[i], 1) for i in range(2)]
    down = [x_step(own[i], -1) for i in range(2)]
    parts = (*own, *up, *down, x_step(up[0], 1), x_step(down[1], -1))

    left_t, gram_parts = kernel(
        functools.partial(gram_terms, n_y), (shape(RANK, d_in), shape(n_f, 8, 128)), [VMEM]
    )(left_parts)

    one, two = out_grad, sibling(out_grad)
    chips = [(0, [(one, 0), (two, 1)])]
    for s in range(1, n_z // 2):
        one, two = turn(one), turn(two)
        chips.append((s, [(one, 0), (two, 1)]))
        chips.append((-s, [(sibling(one), 1), (sibling(two), 0)]))
    s = n_z // 2
    one = turn(one)
    chips.append((s, [(one, 0), (sibling(one), 1)]))

    def parted(held):
        blocks = [block for _, pair in held for block, _ in pair]
        return [by for by, _ in held], blocks, [flip for _, pair in held for _, flip in pair]

    bys, blocks, flips = parted(chips[:5])
    late_bys, last, last_flips = parted(chips[5:])

    def columns(rows, width):
        return pl.BlockSpec((rows, width), lambda n: (0, n))

    def fixed(*dims):
        return pl.BlockSpec(dims, lambda n: (0,) * len(dims))

    width = d_out // n_y
    tall = d_in + 2 * RANK
    wide, late_wide = len(bys) * half, len(late_bys) * half
    total, p_part, turned = kernel(
        functools.partial(fold, bys, flips, late_bys),
        (shape(d_in, d_out), shape(RANK, d_out), shape(tall, late_wide, of=BF16)),
        [SMEM, columns(d_in, width), fixed(RANK, d_in)]
        + [fixed(d_in, half)] * 8
        + [columns(g_rows, width)] * len(blocks),
        flops=2 * tall * wide * d_out,
        grid=(d_out // width,),
        out_specs=(columns(d_in, width), columns(RANK, width), fixed(tall, late_wide)),
        scratch_shapes=[pltpu.VMEM((tall, wide), BF16), pltpu.VMEM((wide, width), BF16)],
    )(code, memory, left_t, *parts, *blocks)
    n_g = n_y * n_f
    piece = kernel(
        functools.partial(last_terms, last_flips),
        shape(n_g, 8, 128),
        [SMEM, columns(RANK, width), fixed(tall, late_wide)]
        + [columns(g_rows, width)] * len(last),
        flops=2 * 64 * late_wide * d_out,
        grid=(d_out // width,),
        out_specs=pl.BlockSpec((n_f, 8, 128), lambda n: (n, 0, 0)),
        scratch_shapes=[pltpu.VMEM((late_wide, width), BF16)],
    )(code, p_part, turned, *last)
    total = kernel(
        functools.partial(fold_last, last_flips),
        shape(d_in, d_out),
        [SMEM, columns(d_in, width), fixed(tall, late_wide)]
        + [columns(g_rows, width)] * len(last),
        flops=2 * d_in * late_wide * d_out,
        grid=(d_out // width,),
        out_specs=columns(d_in, width),
        scratch_shapes=[pltpu.VMEM((late_wide, width), BF16)],
    )(code, total, turned, *last)
    group = ("replica", *fsdp)
    piece = all_sent(piece, group)
    gram_parts = all_sent(gram_parts, fsdp)
    gram = kernel(gram_sum, shape(RANK, RANK), [VMEM])(gram_parts)
    triangle = jnp.linalg.cholesky(gram)
    inverse = jax.scipy.linalg.solve_triangular(triangle, jnp.eye(RANK, dtype=F32), lower=True)
    ortho = dot(left_t, inverse, (((0,), (1,)), ((), ())), lax.Precision.HIGHEST)
    o_hi = lax.reduce_precision(ortho, 8, 7)
    o_lo = ortho - o_hi
    ortho3 = jnp.concatenate([o_hi, o_hi, o_lo], axis=1).astype(BF16)
    piece = kernel(sum_copies, shape(n_g, 8, 128), [VMEM] * 2)(piece, ortho3)
    p_all = all_sent(piece, group).reshape(n_y, n_f, 8, 128)
    new_error, update, factor = kernel(
        functools.partial(finish, n_y),
        (shape(d_in, d_out), shape(d_in, d_out, of=BF16), shape(RANK, d_out)),
        [
            columns(d_in, width),
            fixed(*ortho3.shape),
            fixed(RANK, RANK),
            pl.BlockSpec((1, n_f, 8, 128), lambda n: (n, 0, 0, 0)),
        ],
        flops=2 * 96 * d_in * d_out,
        grid=(d_out // width,),
        out_specs=(columns(d_in, width), columns(d_in, width), columns(RANK, width)),
    )(total, ortho3, inverse, p_all)
    return (new_error[None], update, factor.T)


def solution(mesh):
    devices = mesh.devices.reshape(mesh.shape["replica"], -1, 2, mesh.shape["tensor"])
    mesh = jax.sharding.Mesh(devices, ("replica", "z", "core", "tensor"))
    fsdp = ("z", "core")

    return jax.shard_map(
        body,
        mesh=mesh,
        in_specs=(
            P(("replica", "tensor"), fsdp),
            P(("replica", *fsdp), "tensor"),
            P("replica", fsdp, "tensor"),
            P("tensor", None),
        ),
        out_specs=(P("replica", fsdp, "tensor"), P(fsdp, "tensor"), P("tensor", None)),
        check_vma=False,
    )
```
